256 devices in a mesh: row: 16 (over z_lo, y, core), col: 16 (over z_hi, x).
Axes of the slice: x: 4, y: 4, z: 8 (z_hi: 4, z_lo: 2; z = z_hi * 2 + z_lo), core: 2. Of those that a mesh axis runs over, the one named last changes fastest.
Arguments:
- matrix: bfloat16 [6144, 6144], P('row', 'col'), as said below
- polar_factor: bfloat16 [6144, 6144], P('row', 'col'), as said below
- start_basis: bfloat16 [6144, 6144], P('row', 'col'), may hold values from -0.078125 to 0.078125
Outputs:
- gram_halves: float32 [3072, 6144], P('row', 'col')
- projected: float32 [3072, 6144], P('row', 'col')
The draws below stay inside these ranges and needn't reach their ends.
Inputs may be any that keep to these rules, and one draw needn't show every extreme that they name: `matrix`: symmetric. `polar_factor`: symmetric.
All inputs are finite; a program needn't handle non-finite values.
Results may differ from the reference program's by a relative error of at most 0.017.
Values may be sent and summed in bfloat16 or wider, within the bound.
A program may use at most 64 MiB of HBM per device.

```python
import jax
import jax.numpy as jnp
from jax import lax

N = 6144
K = 3072
BLOCK_ROWS = 384
HALF_BLOCK = 192
N_ROW = 16
N_COL = 16


def spectral_parts(key):
    base = jax.random.fold_in(key, 7)
    first, second, third = jax.random.split(base, 3)
    normal_draw = jax.random.normal(first, (N, N), jnp.float32)
    orthogonal, unused = jnp.linalg.qr(normal_draw)
    magnitude = jax.random.uniform(second, (N,), jnp.float32, 0.2, 2.0)
    signs = jnp.where(jnp.arange(N) < K, 1.0, -1.0).astype(jnp.float32)
    errors = jax.random.uniform(third, (N,), jnp.float32, 0.0, 0.3)
    return (orthogonal, signs * magnitude, signs * (1.0 - errors))


def symmetric_from(orthogonal, values):
    built = jnp.dot(orthogonal * values[None, :], orthogonal.T, precision=lax.Precision.HIGHEST)
    return 0.5 * (built + built.T)


def draw_matrix(key, part):
    orthogonal, eigen, polar = spectral_parts(key)
    return symmetric_from(orthogonal, eigen).astype(jnp.bfloat16)


def draw_polar_factor(key, part):
    orthogonal, eigen, polar = spectral_parts(key)
    return symmetric_from(orthogonal, polar).astype(jnp.bfloat16)


def block_scale(own_key, shape, pieces, smallest, top_value):
    gain, own = 1.0, jax.random.fold_in(own_key, 6)
    for dim, blocks in pieces:
        heights = jnp.exp(jax.random.uniform(jax.random.fold_in(own, dim), (blocks,), jnp.float32, smallest / len(pieces), top_value / len(pieces)))
        gain = gain * jnp.repeat(heights, shape[dim] // blocks).reshape([-1 if axis == dim else 1 for axis in range(len(shape))])
    return gain


def noise(stream_key, dims, width, bound, cuts=(), dtype=jnp.bfloat16):
    factor_of = block_scale(stream_key, dims, cuts, -0.22, 0.18) if cuts else 1.0
    array = jax.random.normal(stream_key, dims, jnp.float32) * width * factor_of
    return jnp.minimum(jnp.maximum(array, -bound), bound).astype(dtype)


def setup_inputs(seed: int = 0) -> dict:
    splits = jax.random.split(jax.random.key(seed), 4)
    matrix = draw_matrix(jax.random.fold_in(splits[3], 71), 0)
    polar_factor = draw_polar_factor(jax.random.fold_in(splits[3], 71), 0)
    start_basis = noise(splits[2], (N, 2 * K), N ** -0.5, 0.078125, ((0, 16), (1, 16)))
    return dict(matrix=matrix, polar_factor=polar_factor, start_basis=start_basis)


def add_block(running, blocks):
    left, right = blocks
    term = jnp.dot(left.T.astype(jnp.float32), right.astype(jnp.float32), preferred_element_type=jnp.float32).astype(jnp.bfloat16)
    term = lax.optimization_barrier(term)
    return (running + term.astype(jnp.float32), None)

def reference(matrix, polar_factor, start_basis):
    product = jnp.dot(polar_factor.astype(jnp.float32), start_basis.astype(jnp.float32), preferred_element_type=jnp.float32)
    signs = jnp.where(jnp.arange(2 * K) // HALF_BLOCK % 2 == 0, 1.0, -1.0).astype(jnp.float32)
    basis = ((start_basis.astype(jnp.float32) + signs * product) * 0.5).astype(jnp.bfloat16)
    image = jnp.dot(matrix.astype(jnp.float32), basis.astype(jnp.float32), preferred_element_type=jnp.float32).astype(jnp.bfloat16)
    basis_split = basis.reshape(N, N_COL, 2, HALF_BLOCK)
    image_split = image.reshape(N, N_COL, 2, HALF_BLOCK)
    grams = []
    projections = []
    for which in range(2):
        basis_half = basis_split[:, :, which, :].reshape(N, K)
        image_half = image_split[:, :, which, :].reshape(N, K)
        joined = jnp.concatenate([basis_half, image_half], axis=1)
        left_blocks = basis_half.reshape(N_ROW, BLOCK_ROWS, K)
        right_blocks = joined.reshape(N_ROW, BLOCK_ROWS, 2 * K)
        summed, unused = lax.scan(add_block, jnp.zeros((K, 2 * K), jnp.float32), (left_blocks, right_blocks))
        grams.append(summed[:, :K].reshape(K, N_COL, HALF_BLOCK))
        projections.append(summed[:, K:].reshape(K, N_COL, HALF_BLOCK))
    gram_halves = jnp.stack(grams, axis=2).reshape(K, 2 * K)
    projected = jnp.stack(projections, axis=2).reshape(K, 2 * K)
    return (gram_halves, projected)
```

```python
import jax
import jax.numpy as jnp
from jax import lax
from jax.experimental import pallas as pl
from jax.experimental.pallas import tpu as pltpu
from jax.sharding import PartitionSpec as P

BF16 = jnp.bfloat16
F32 = jnp.float32
SIDES = (-1, 1)
N_SEMS = 178
X_ROWS = 64


def kernel(
    p_in, m_in, s_in, gram_out, proj_out,
    p_panel, m_panel, t_panel, s_panel, b_panel, i_panel,
    turned, total, total2, send_sems, recv_sems,
):
    width = s_in.shape[0]
    half = width // 2
    row, col = lax.axis_index("row"), lax.axis_index("col")
    core, y, zl = row % 2, (row // 2) % 4, row // 8
    x, zh = col % 4, col // 4

    def device(x=x, y=y, zh=zh, zl=zl, core=core):
        return ((zl * 4 + y) * 2 + core, zh * 4 + x)

    def near(axis, step):
        if axis == "x":
            return device(x=(x + step + 4) % 4)
        if axis == "z":
            return device(zh=(zh + step + 4) % 4)
        return device(y=(y + step + 4) % 4)

    peer = device(zl=1 - zl)
    sibling = device(core=1 - core)
    mirror = (col, row)
    sends = []
    slots = {}

    def slot(key):
        return slots.setdefault(key, len(slots))

    def copy(src, dst, to, key):
        return pltpu.make_async_remote_copy(
            src_ref=src, dst_ref=dst,
            send_sem=send_sems.at[slot(key)], recv_sem=recv_sems.at[slot(key)],
            device_id=to, device_id_type=pl.DeviceIdType.MESH,
        )

    def send(src, dst, to, key):
        one = copy(src, dst, to, key)
        one.start()
        sends.append(one)

    def arrive(ref, key):
        copy(ref, ref, sibling, key).wait_recv()

    class Panel:
        def __init__(self, name, panel, own, at, n, first, second):
            self.name, self.panel, self.own = name, panel, own
            self.whole = pl.ds(at, n)
            self.lower, self.upper = pl.ds(at, n // 2), pl.ds(at + n // 2, n // 2)
            self.first, self.second = first, second

        def part(self, df, ds, rows):
            dz, dx = (df, ds) if self.first == "z" else (ds, df)
            return self.panel.at[((zh + dz + 4) % 4) * 4 + (x + dx + 4) % 4, rows]

        def source(self, df, ds, rows):
            return self.own.at[rows] if df == 0 and ds == 0 else self.part(df, ds, rows)

        def out(self, df, ds, rows, axis, step, *key):
            send(self.source(df, ds, rows), self.part(df, ds, rows), near(axis, step), (self.name,) + key)

        def wait(self, df, ds, rows, *key):
            arrive(self.part(df, ds, rows), (self.name,) + key)

        def f1(self):
            for side in SIDES:
                self.out(0, 0, self.whole, self.first, -side, "f", side)

        def f2(self):
            for side in SIDES:
                self.wait(side, 0, self.whole, "f", side)
                rows = self.lower if side == -1 else self.upper
                self.out(side, 0, rows, self.first, -side, "ff", side)

        def f3(self):
            for side in SIDES:
                self.wait(2, 0, self.lower if side == -1 else self.upper, "ff", side)

        def s1(self, d):
            for side in SIDES:
                self.out(d, 0, self.whole, self.second, -side, "s", d, side)

        def s2(self, d):
            for side in SIDES:
                self.wait(d, side, self.whole, "s", d, side)
                rows = self.lower if side == -1 else self.upper
                self.out(d, side, rows, self.second, -side, "ss", d, side)

        def s3(self, d):
            for side in SIDES:
                self.wait(d, 2, self.lower if side == -1 else self.upper, "ss", d, side)

    class Column:
        def __init__(self, name, panel, own):
            self.name, self.panel, self.own = name, panel, own
            self.whole = pl.ds(0, width)
            self.lower, self.upper = pl.ds(0, half), pl.ds(half, half)

        def part(self, dz, dy, rows, of=core):
            at_z = zl if dz == 0 else 1 - zl
            return self.panel.at[(at_z * 4 + (y + dy + 4) % 4) * 2 + of, rows]

        def out(self, dz, dy, rows, to, *key):
            own = dz == 0 and dy == 0
            src = self.own.at[rows] if own else self.part(dz, dy, rows)
            send(src, self.part(dz, dy, rows), to, (self.name,) + key)

        def wait(self, dz, dy, rows, *key):
            arrive(self.part(dz, dy, rows), (self.name,) + key)

        def r1(self):
            for side in SIDES:
                self.out(0, 0, self.whole, near("y", -side), "y", 0, side)
            self.out(0, 0, self.whole, peer, "z")
            self.out(0, 0, self.whole, sibling, "d", 0, 0)

        def rz(self):
            self.wait(1, 0, self.whole, "z")
            for side in SIDES:
                self.out(1, 0, self.whole, near("y", -side), "y", 1, side)
            self.out(1, 0, self.whole, sibling, "d", 1, 0)

        def r2(self, q):
            for side in SIDES:
                self.wait(q, side, self.whole, "y", q, side)
                rows = self.lower if side == -1 else self.upper
                self.out(q, side, rows, near("y", -side), "yy", q, side)
                self.out(q, side, self.whole, sibling, "d", q, side)

        def r3(self, q):
            for side in SIDES:
                rows = self.lower if side == -1 else self.upper
                self.wait(q, 2, rows, "yy", q, side)
                self.out(q, 2, rows, sibling, "dd", q, side)

        def r4(self):
            other = 1 - core
            for q in (0, 1):
                for dy in (0,) + SIDES:
                    arrive(self.part(q, dy, self.whole, other), (self.name, "d", q, dy))
                for side in SIDES:
                    rows = self.lower if side == -1 else self.upper
                    arrive(self.part(q, 2, rows, other), (self.name, "dd", q, side))

    def two_ways(name, panel, own):
        split = width - X_ROWS
        return (
            Panel(name + "a", panel, own, 0, split, "z", "x"),
            Panel(name + "b", panel, own, split, X_ROWS, "x", "z"),
        )

    def begin(ways):
        a, b = ways
        a.f1()
        b.f1()
        a.s1(0)

    def add_group(dz, left, rights):
        base = ((zh + dz + 4) % 4) * 4

        @pl.loop(0, 4)
        def _(j):
            for right, into in rights:
                into[...] += jnp.dot(left[base + j], right[base + j], preferred_element_type=F32)

    def phase(ways, column, left, rights, then):
        a, b = ways
        b.f2()
        a.s2(0)
        column.r2(0)
        b.f3()
        a.f2()
        a.s1(-1)
        a.s1(1)
        for d in (0, -1, 1, 2):
            b.s1(d)
        column.r3(0)
        a.s2(-1)
        column.rz()
        a.s2(1)
        a.f3()
        a.s1(2)
        column.r2(1)
        for d in (0, -1, 1):
            b.s2(d)
        column.r3(1)
        a.s2(2)
        b.s2(2)
        then()
        a.s3(0)
        column.r4()
        add_group(0, left, rights)
        a.s3(-1)
        add_group(-1, left, rights)
        a.s3(1)
        add_group(1, left, rights)
        a.s3(2)
        for d in (0, -1, 1, 2):
            b.s3(d)
        add_group(2, left, rights)

    barrier = pltpu.get_barrier_semaphore()
    partners = [near(axis, step) for axis in "xyz" for step in SIDES] + [peer, sibling]
    for partner in partners:
        pl.semaphore_signal(barrier, inc=1, device_id=partner, device_id_type=pl.DeviceIdType.MESH)

    @pl.when(row != col)
    def _():
        pl.semaphore_signal(barrier, inc=1, device_id=mirror, device_id_type=pl.DeviceIdType.MESH)
        pl.semaphore_wait(barrier, len(partners) + 1)

    @pl.when(row == col)
    def _():
        pl.semaphore_wait(barrier, len(partners))

    polar = two_ways("p", p_panel, p_in)
    matrix = two_ways("m", m_panel, m_in)
    turned_rows = two_ways("t", t_panel, t_panel.at[col])
    start = Column("s", s_panel, s_in)
    basis = Column("b", b_panel, b_panel.at[row])
    image = Column("i", i_panel, i_panel.at[row])

    begin(polar)
    start.r1()
    p_panel[col] = p_in[...]
    m_panel[col] = m_in[...]
    s_panel[row] = s_in[...]
    total[...] = jnp.zeros_like(total)
    phase(polar, start, p_panel, ((s_panel, total),), lambda: begin(matrix))

    first = lax.broadcasted_iota(jnp.int32, (width, width), 1) < half
    product = total[...]
    value = ((s_in[...].astype(F32) + jnp.where(first, product, -product)) * 0.5).astype(BF16)
    b_panel[row] = value
    turned[...] = jnp.transpose(value.astype(F32)).astype(BF16)
    total[...] = jnp.zeros_like(total)
    basis.r1()
    to_mirror = copy(turned, t_panel.at[row], mirror, "turn")

    @pl.when(row != col)
    def _():
        to_mirror.start()

    @pl.when(row == col)
    def _():
        t_panel[col] = turned[...]

    def begin_turned():
        @pl.when(row != col)
        def _():
            copy(t_panel.at[col], t_panel.at[col], mirror, "turn").wait_recv()

        begin(turned_rows)

    phase(matrix, basis, m_panel, ((b_panel, total),), begin_turned)

    i_panel[row] = total[...].astype(BF16)
    total[...] = jnp.zeros_like(total)
    total2[...] = jnp.zeros_like(total2)
    image.r1()
    phase(turned_rows, image, t_panel, ((b_panel, total), (i_panel, total2)), lambda: None)

    keep = lax.broadcasted_iota(jnp.int32, (half, width), 1) < half
    gram_out[...] = jnp.where(keep, total[:half], total[half:])
    proj_out[...] = jnp.where(keep, total2[:half], total2[half:])

    for one in sends:
        one.wait_send()

    @pl.when(row != col)
    def _():
        to_mirror.wait_send()


def per_device(matrix, polar_factor, start_basis):
    width = start_basis.shape[0]
    blocks = 16
    vmem = pl.BlockSpec(memory_space=pltpu.VMEM)
    out = jax.ShapeDtypeStruct((width // 2, width), F32)
    panel = pltpu.VMEM((blocks, width, width), BF16)
    return pl.pallas_call(
        kernel,
        out_shape=(out, out),
        in_specs=[vmem] * 3,
        out_specs=(vmem, vmem),
        scratch_shapes=[panel] * 6
        + [
            pltpu.VMEM((width, width), BF16),
            pltpu.VMEM((width, width), F32),
            pltpu.VMEM((width, width), F32),
            pltpu.SemaphoreType.DMA((N_SEMS,)),
            pltpu.SemaphoreType.DMA((N_SEMS,)),
        ],
        compiler_params=pltpu.CompilerParams(
            collective_id=0, has_side_effects=True, vmem_limit_bytes=48 * 1024 * 1024
        ),
    )(polar_factor, matrix, start_basis)


def solution(mesh):
    return jax.shard_map(
        per_device,
        mesh=mesh,
        in_specs=(P("row", "col"), P("row", "col"), P("row", "col")),
        out_specs=(P("row", "col"), P("row", "col")),
        check_vma=False,
    )
```

```python
import jax
import jax.numpy as jnp
from jax import lax
from jax.experimental import pallas as pl
from jax.experimental.pallas import tpu as pltpu
from jax.sharding import PartitionSpec as P

BF16 = jnp.bfloat16
F32 = jnp.float32
SIDES = (-1, 1)
N_SEMS = 118
X_ROWS = (64, 64, 64)


def kernel(
    p_in, m_in, s_in, gram_out, proj_out,
    p_panel, m_panel, t_panel, s_panel, b_panel, i_panel,
    turned, total, total2, send_sems, recv_sems,
):
    width, blocks = total.shape[0], p_panel.shape[0]
    half = width // 2
    row, col = lax.axis_index("row"), lax.axis_index("col")
    core, y, zl = row % 2, (row // 2) % 4, row // 8
    x, zh = col % 4, col // 4

    def device(x=x, y=y, zh=zh, zl=zl, core=core):
        return ((zl * 4 + y) * 2 + core, zh * 4 + x)

    def near(axis, step):
        if axis == "x":
            return device(x=(x + step + 4) % 4)
        if axis == "z":
            return device(zh=(zh + step + 4) % 4)
        return device(y=(y + step + 4) % 4)

    peer = device(zl=1 - zl)
    sibling = device(core=1 - core)
    mirror = (col, row)
    slots = {}

    def slot(key):
        return slots.setdefault(key, len(slots))

    def copy(src, dst, to, key):
        return pltpu.make_async_remote_copy(
            src_ref=src, dst_ref=dst,
            send_sem=send_sems.at["psmbtiu".index(key[0][0])], recv_sem=recv_sems.at[slot(key)],
            device_id=to, device_id_type=pl.DeviceIdType.MESH,
        )

    def send(src, dst, to, key):
        copy(src, dst, to, key).start()

    def arrive(ref, key):
        copy(ref, ref, sibling, key).wait_recv()

    def pairs(ds):
        return [(d, side) for d in ds or (0, -1, 1, 2) for side in SIDES]

    inputs = {"pa": p_in, "pb": p_in, "ma": m_in, "mb": m_in, "s": s_in}

    class Panel:
        def __init__(self, name, panel, at, n, first, second):
            self.name, self.panel = name, panel
            self.whole = pl.ds(at, n)
            self.lower, self.upper = pl.ds(at, n // 2), pl.ds(at + n // 2, n // 2)
            self.first, self.second = first, second

        def part(self, df, ds, rows):
            dz, dx = (df, ds) if self.first == "z" else (ds, df)
            return self.panel.at[((zh + dz + 4) % 4) * 4 + (x + dx + 4) % 4, rows]

        def out(self, df, ds, rows, axis, step, *key):
            src = self.part(df, ds, rows)
            if df == 0 and ds == 0 and self.name in inputs:
                src = inputs[self.name].at[rows]
            send(src, self.part(df, ds, rows), near(axis, step), (self.name,) + key)

        def wait(self, df, ds, rows, *key):
            arrive(self.part(df, ds, rows), (self.name,) + key)

        def f1(self):
            for side in SIDES:
                self.out(0, 0, self.whole, self.first, -side, "f", side)

        def f2(self):
            for side in SIDES:
                self.wait(side, 0, self.whole, "f", side)
                rows = self.lower if side == -1 else self.upper
                self.out(side, 0, rows, self.first, -side, "ff")

        def f3(self):
            self.wait(2, 0, self.whole, "ff")

        def s1(self, *ds):
            for d, side in pairs(ds):
                self.out(d, 0, self.whole, self.second, -side, "s", d, side)

        def s2(self, *ds):
            for d, side in pairs(ds):
                self.wait(d, side, self.whole, "s", d, side)
                rows = self.lower if side == -1 else self.upper
                self.out(d, side, rows, self.second, -side, "ss", d)

        def s3(self, *ds):
            for d in ds or (0, -1, 1, 2):
                self.wait(d, 2, self.whole, "ss", d)

    class Column:
        def __init__(self, name, panel):
            self.name, self.panel = name, panel
            self.whole = pl.ds(0, width)
            self.lower, self.upper = pl.ds(0, half), pl.ds(half, half)

        def part(self, dz, dy, rows, of=core):
            at_z = zl if dz == 0 else 1 - zl
            return self.panel.at[(at_z * 4 + (y + dy + 4) % 4) * 2 + of, rows]

        def out(self, dz, dy, rows, to, *key):
            src = self.part(dz, dy, rows)
            if dz == 0 and dy == 0 and self.name in inputs:
                src = inputs[self.name].at[rows]
            send(src, self.part(dz, dy, rows), to, (self.name,) + key)

        def wait(self, dz, dy, rows, *key):
            arrive(self.part(dz, dy, rows), (self.name,) + key)

        def r1(self):
            for side in SIDES:
                self.out(0, 0, self.whole, near("y", -side), "y", 0, side)
            self.out(0, 0, self.whole, peer, "z")
            self.out(0, 0, self.whole, sibling, "d", 0)

        def rz(self):
            self.wait(1, 0, self.whole, "z")
            for side in SIDES:
                self.out(1, 0, self.whole, near("y", -side), "y", 1, side)
            self.out(1, 0, self.whole, sibling, "d", 1)

        def r2(self, q):
            for side in SIDES:
                self.wait(q, side, self.whole, "y", q, side)
                rows = self.lower if side == -1 else self.upper
                self.out(q, side, rows, near("y", -side), "yy", q)
                self.out(q, side, self.whole, sibling, "d", q)

        def r3(self, q):
            self.wait(q, 2, self.whole, "yy", q)
            self.out(q, 2, self.whole, sibling, "d", q)

        def r4(self, *qs):
            for q in qs or (0, 1):
                arrive(self.panel.at[pl.ds(0, 4)], (self.name, "d", q))

    def two_ways(name, panel, rows):
        split = width - rows
        return (
            Panel(name + "a", panel, 0, split, "z", "x"),
            Panel(name + "b", panel, split, rows, "x", "z"),
        )

    def add_group(dz, left, right, into):
        base = ((zh + dz + 4) % 4) * 4

        @pl.loop(0, 4)
        def _(j):
            into[...] += jnp.dot(left[base + j], right[base + j], preferred_element_type=F32)

    barrier = pltpu.get_barrier_semaphore()
    partners = [near(axis, step) for axis in "xyz" for step in SIDES] + [peer, sibling]
    for partner in partners:
        pl.semaphore_signal(barrier, inc=1, device_id=partner, device_id_type=pl.DeviceIdType.MESH)

    @pl.when(row != col)
    def _():
        pl.semaphore_signal(barrier, inc=1, device_id=mirror, device_id_type=pl.DeviceIdType.MESH)
        pl.semaphore_wait(barrier, len(partners) + 1)

    @pl.when(row == col)
    def _():
        pl.semaphore_wait(barrier, len(partners))

    pa, pb = two_ways("p", p_panel, X_ROWS[0])
    ma, mb = two_ways("m", m_panel, X_ROWS[1])
    ta, tb = two_ways("t", t_panel, X_ROWS[2])
    start = Column("s", s_panel)
    basis = Column("b", b_panel)
    image = Column("i", i_panel)
    to_mirror = copy(turned, t_panel.at[row], mirror, ("u",))

    pa.f1()
    pb.f1()
    pa.s1(0)
    start.r1()
    p_panel[col] = p_in[...]
    s_panel[row] = s_in[...]
    m_panel[col] = m_in[...]
    total[...] = jnp.zeros_like(total)
    pb.f2()
    pa.s2(0)
    start.r2(0)
    pb.f3()
    pa.f2()
    pa.s1(-1)
    pa.s1(1)
    pa.s2(-1)
    start.rz()
    pb.s1()
    pa.s2(1)
    pa.f3()
    pa.s1(2)
    pb.s2(0)
    start.r2(1)
    pb.s2(-1, 1, 2)
    ma.f1()
    pa.s2(2)
    mb.f1()
    ma.s1(0)
    start.r3(0)
    start.r3(1)
    start.r4()
    for d in (0, -1, 1):
        pa.s3(d)
        add_group(d, p_panel, s_panel, total)
    pa.s3(2)
    pb.s3()
    add_group(2, p_panel, s_panel, total)

    first = lax.broadcasted_iota(jnp.int32, (width, width), 1) < half
    product = total[...]
    value = ((s_panel[row].astype(F32) + jnp.where(first, product, -product)) * 0.5).astype(BF16)
    b_panel[row] = value
    turned[...] = jnp.transpose(value.astype(F32)).astype(BF16)
    total[...] = jnp.zeros_like(total)
    basis.r1()

    @pl.when(row != col)
    def _():
        to_mirror.start()

    @pl.when(row == col)
    def _():
        t_panel[col] = turned[...]

    mb.f2()
    ma.s2(0)
    ma.f2()
    ma.s1(-1)
    ma.s1(1)
    mb.f3()
    basis.r2(0)
    basis.rz()
    mb.s1()
    ma.s2(-1)
    ma.s2(1)
    ma.f3()
    ma.s1(2)
    mb.s2(0)
    basis.r2(1)
    mb.s2(-1, 1, 2)

    @pl.when(row != col)
    def _():
        copy(t_panel.at[col], t_panel.at[col], mirror, ("u",)).wait_recv()

    ta.f1()
    ma.s2(2)
    tb.f1()
    ta.s1(0)
    basis.r3(0)
    basis.r3(1)
    basis.r4()
    for d in (0, -1, 1):
        ma.s3(d)
        add_group(d, m_panel, b_panel, total)
    ma.s3(2)
    mb.s3()
    add_group(2, m_panel, b_panel, total)
    i_panel[row] = total[...].astype(BF16)
    total[...] = jnp.zeros_like(total)
    total2[...] = jnp.zeros_like(total2)
    image.r1()
    tb.f2()
    ta.s2(0)
    ta.f2()
    ta.s1(-1)
    ta.s1(1)
    tb.f3()
    image.r2(0)
    image.rz()
    tb.s1()
    ta.s2(-1)
    ta.s2(1)
    ta.f3()
    ta.s1(2)
    tb.s2(0)
    image.r2(1)
    tb.s2(-1, 1, 2)
    ta.s2(2)
    image.r3(0)
    for d in (0, -1, 1):
        ta.s3(d)
        add_group(d, t_panel, b_panel, total)
    image.r3(1)
    image.r4()
    for d in (0, -1, 1):
        add_group(d, t_panel, i_panel, total2)
    ta.s3(2)
    tb.s3()
    add_group(2, t_panel, b_panel, total)
    add_group(2, t_panel, i_panel, total2)

    assert len(slots) == N_SEMS
    keep = lax.broadcasted_iota(jnp.int32, (half, width), 1) < half
    gram_out[...] = jnp.where(keep, total[:half], total[half:])
    proj_out[...] = jnp.where(keep, total2[:half], total2[half:])

    for panel, name in ((p_panel, "p"), (s_panel, "s"), (m_panel, "m"), (b_panel, "b"), (t_panel, "t"), (i_panel, "i")):
        sent = panel.at[pl.ds(0, blocks - 1)]
        copy(sent, sent, sibling, (name + "a", "f", 1) if name in "pmt" else (name, "z")).wait_send()

    @pl.when(row != col)
    def _():
        to_mirror.wait_send()


def per_device(matrix, polar_factor, start_basis):
    width = start_basis.shape[0]
    blocks = 16
    vmem = pl.BlockSpec(memory_space=pltpu.VMEM)
    out = jax.ShapeDtypeStruct((width // 2, width), F32)
    panel = pltpu.VMEM((blocks, width, width), BF16)
    return pl.pallas_call(
        kernel,
        out_shape=(out, out),
        in_specs=[vmem] * 3,
        out_specs=(vmem, vmem),
        scratch_shapes=[panel] * 6
        + [
            pltpu.VMEM((width, width), BF16),
            pltpu.VMEM((width, width), F32),
            pltpu.VMEM((width, width), F32),
            pltpu.SemaphoreType.DMA((7,)),
            pltpu.SemaphoreType.DMA((N_SEMS,)),
        ],
        compiler_params=pltpu.CompilerParams(
            collective_id=0, has_side_effects=True, vmem_limit_bytes=48 * 1024 * 1024
        ),
    )(polar_factor, matrix, start_basis)


def solution(mesh):
    return jax.shard_map(
        per_device,
        mesh=mesh,
        in_specs=(P("row", "col"), P("row", "col"), P("row", "col")),
        out_specs=(P("row", "col"), P("row", "col")),
        check_vma=False,
    )
```

```python
import jax
import jax.numpy as jnp
from jax import lax
from jax.experimental import pallas as pl
from jax.experimental.pallas import tpu as pltpu
from jax.sharding import PartitionSpec as P

BF16 = jnp.bfloat16
F32 = jnp.float32
SIDES = (-1, 1)
N_SEMS = 118
X_ROWS = (64, 64, 64)


def kernel(
    p_in, m_in, s_in, gram_out, proj_out,
    p_panel, m_panel, t_panel, s_panel, b_panel, i_panel,
    turned, total, total2, send_sems, recv_sems,
):
    width, blocks = total.shape[0], p_panel.shape[0]
    half = width // 2
    row, col = lax.axis_index("row"), lax.axis_index("col")
    core, y, zl = row % 2, (row // 2) % 4, row // 8
    x, zh = col % 4, col // 4

    def device(x=x, y=y, zh=zh, zl=zl, core=core):
        return ((zl * 4 + y) * 2 + core, zh * 4 + x)

    def near(axis, step):
        if axis == "x":
            return device(x=(x + step + 4) % 4)
        if axis == "z":
            return device(zh=(zh + step + 4) % 4)
        return device(y=(y + step + 4) % 4)

    peer = device(zl=1 - zl)
    sibling = device(core=1 - core)
    mirror = (col, row)
    slots = {}

    def slot(key):
        return slots.setdefault(key, len(slots))

    def copy(src, dst, to, key):
        return pltpu.make_async_remote_copy(
            src_ref=src, dst_ref=dst,
            send_sem=send_sems.at["psmbtiu".index(key[0][0])], recv_sem=recv_sems.at[slot(key)],
            device_id=to, device_id_type=pl.DeviceIdType.MESH,
        )

    def send(src, dst, to, key):
        copy(src, dst, to, key).start()

    def arrive(ref, key):
        copy(ref, ref, sibling, key).wait_recv()

    def pairs(ds):
        return [(d, side) for d in ds or (0, -1, 1, 2) for side in SIDES]

    inputs = {"pa": p_in, "pb": p_in, "ma": m_in, "mb": m_in, "s": s_in}

    class Panel:
        def __init__(self, name, panel, at, n, first, second):
            self.name, self.panel = name, panel
            self.whole = pl.ds(at, n)
            self.lower, self.upper = pl.ds(at, n // 2), pl.ds(at + n // 2, n // 2)
            self.first, self.second = first, second

        def part(self, df, ds, rows):
            dz, dx = (df, ds) if self.first == "z" else (ds, df)
            return self.panel.at[((zh + dz + 4) % 4) * 4 + (x + dx + 4) % 4, rows]

        def out(self, df, ds, rows, axis, step, *key):
            src = self.part(df, ds, rows)
            if df == 0 and ds == 0 and self.name in inputs:
                src = inputs[self.name].at[rows]
            send(src, self.part(df, ds, rows), near(axis, step), (self.name,) + key)

        def wait(self, df, ds, rows, *key):
            arrive(self.part(df, ds, rows), (self.name,) + key)

        def f1(self):
            for side in SIDES:
                self.out(0, 0, self.whole, self.first, -side, "f", side)

        def f2(self):
            for side in SIDES:
                self.wait(side, 0, self.whole, "f", side)
                rows = self.lower if side == -1 else self.upper
                self.out(side, 0, rows, self.first, -side, "ff")

        def f3(self):
            self.wait(2, 0, self.whole, "ff")

        def s1(self, *ds):
            for d, side in pairs(ds):
                self.out(d, 0, self.whole, self.second, -side, "s", d, side)

        def s2(self, *ds):
            for d, side in pairs(ds):
                self.wait(d, side, self.whole, "s", d, side)
                rows = self.lower if side == -1 else self.upper
                self.out(d, side, rows, self.second, -side, "ss", d)

        def s3(self, *ds):
            for d in ds or (0, -1, 1, 2):
                self.wait(d, 2, self.whole, "ss", d)

    class Column:
        def __init__(self, name, panel):
            self.name, self.panel = name, panel
            self.whole = pl.ds(0, width)
            self.lower, self.upper = pl.ds(0, half), pl.ds(half, half)

        def part(self, dz, dy, rows, of=core):
            at_z = zl if dz == 0 else 1 - zl
            return self.panel.at[(at_z * 4 + (y + dy + 4) % 4) * 2 + of, rows]

        def out(self, dz, dy, rows, to, *key):
            src = self.part(dz, dy, rows)
            if dz == 0 and dy == 0 and self.name in inputs:
                src = inputs[self.name].at[rows]
            send(src, self.part(dz, dy, rows), to, (self.name,) + key)

        def wait(self, dz, dy, rows, *key):
            arrive(self.part(dz, dy, rows), (self.name,) + key)

        def r1(self):
            for side in SIDES:
                self.out(0, 0, self.whole, near("y", -side), "y", 0, side)
            self.out(0, 0, self.whole, peer, "z")
            self.out(0, 0, self.whole, sibling, "d", 0)

        def rz(self):
            self.wait(1, 0, self.whole, "z")
            for side in SIDES:
                self.out(1, 0, self.whole, near("y", -side), "y", 1, side)
            self.out(1, 0, self.whole, sibling, "d", 1)

        def r2(self, q):
            for side in SIDES:
                self.wait(q, side, self.whole, "y", q, side)
                rows = self.lower if side == -1 else self.upper
                self.out(q, side, rows, near("y", -side), "yy", q)
                self.out(q, side, self.whole, sibling, "d", q)

        def r3(self, q):
            self.wait(q, 2, self.whole, "yy", q)
            self.out(q, 2, self.whole, sibling, "d", q)

        def r4(self, *qs):
            for q in qs or (0, 1):
                arrive(self.panel.at[pl.ds(0, 4)], (self.name, "d", q))

    def two_ways(name, panel, rows):
        split = width - rows
        return (
            Panel(name + "a", panel, 0, split, "z", "x"),
            Panel(name + "b", panel, split, rows, "x", "z"),
        )

    def add_group(dz, left, right, into):
        base = ((zh + dz + 4) % 4) * 4

        @pl.loop(0, 4)
        def _(j):
            into[...] += jnp.dot(left[base + j], right[base + j], preferred_element_type=F32)

    barrier = pltpu.get_barrier_semaphore()
    partners = [near(axis, step) for axis in "xyz" for step in SIDES] + [peer, sibling]
    for partner in partners:
        pl.semaphore_signal(barrier, inc=1, device_id=partner, device_id_type=pl.DeviceIdType.MESH)

    @pl.when(row != col)
    def _():
        pl.semaphore_signal(barrier, inc=1, device_id=mirror, device_id_type=pl.DeviceIdType.MESH)
        pl.semaphore_wait(barrier, len(partners) + 1)

    @pl.when(row == col)
    def _():
        pl.semaphore_wait(barrier, len(partners))

    pa, pb = two_ways("p", p_panel, X_ROWS[0])
    ma, mb = two_ways("m", m_panel, X_ROWS[1])
    ta, tb = two_ways("t", t_panel, X_ROWS[2])
    start = Column("s", s_panel)
    basis = Column("b", b_panel)
    image = Column("i", i_panel)
    to_mirror = copy(turned, t_panel.at[row], mirror, ("u",))

    pa.f1()
    pb.f1()
    pa.s1(0)
    start.r1()
    p_panel[col] = p_in[...]
    s_panel[row] = s_in[...]
    m_panel[col] = m_in[...]
    total[...] = jnp.zeros_like(total)
    pb.f2()
    pa.s2(0)
    start.r2(0)
    pb.f3()
    pa.f2()
    pa.s1(-1)
    pa.s1(1)
    pa.s2(-1)
    start.rz()
    pb.s1()
    pa.s2(1)
    pa.f3()
    pa.s1(2)
    start.r3(0)
    pb.s2(0)
    start.r2(1)
    pb.s2(-1, 1, 2)
    ma.f1()
    pa.s2(2)
    mb.f1()
    ma.s1(0)
    start.r3(1)
    start.r4(0)
    start.r4(1)
    for d in (0, -1, 1):
        pa.s3(d)
        add_group(d, p_panel, s_panel, total)
    pa.s3(2)
    pb.s3()
    add_group(2, p_panel, s_panel, total)

    first = lax.broadcasted_iota(jnp.int32, (width, width), 1) < half
    product = total[...]
    value = ((s_panel[row].astype(F32) + jnp.where(first, product, -product)) * 0.5).astype(BF16)
    b_panel[row] = value
    turned[...] = jnp.transpose(value.astype(F32)).astype(BF16)
    total[...] = jnp.zeros_like(total)
    basis.r1()

    @pl.when(row != col)
    def _():
        to_mirror.start()

    @pl.when(row == col)
    def _():
        t_panel[col] = turned[...]

    mb.f2()
    ma.s2(0)
    ma.f2()
    ma.s1(-1)
    ma.s1(1)
    mb.f3()
    basis.r2(0)
    basis.rz()
    mb.s1()
    ma.s2(-1)
    ma.s2(1)
    ma.f3()
    ma.s1(2)
    basis.r3(0)
    mb.s2(0)
    basis.r2(1)
    mb.s2(-1, 1, 2)

    @pl.when(row != col)
    def _():
        copy(t_panel.at[col], t_panel.at[col], mirror, ("u",)).wait_recv()

    ta.f1()
    basis.r3(1)
    ma.s2(2)
    tb.f1()
    ta.s1(0)
    basis.r4(0)
    basis.r4(1)
    for d in (0, -1, 1):
        ma.s3(d)
        add_group(d, m_panel, b_panel, total)
    ma.s3(2)
    mb.s3()
    add_group(2, m_panel, b_panel, total)
    i_panel[row] = total[...].astype(BF16)
    total[...] = jnp.zeros_like(total)
    total2[...] = jnp.zeros_like(total2)
    image.r1()
    tb.f2()
    ta.s2(0)
    ta.f2()
    ta.s1(-1)
    ta.s1(1)
    tb.f3()
    image.r2(0)
    image.rz()
    tb.s1()
    ta.s2(-1)
    ta.s3(0)
    add_group(0, t_panel, b_panel, total)
    ta.s2(1)
    ta.f3()
    ta.s1(2)
    image.r3(0)
    image.r2(1)
    tb.s2()
    for d in (-1, 1):
        ta.s3(d)
        add_group(d, t_panel, b_panel, total)
    image.r3(1)
    ta.s2(2)
    image.r4()
    for d in (0, -1, 1):
        add_group(d, t_panel, i_panel, total2)
    ta.s3(2)
    tb.s3()
    add_group(2, t_panel, b_panel, total)
    add_group(2, t_panel, i_panel, total2)

    assert len(slots) == N_SEMS
    keep = lax.broadcasted_iota(jnp.int32, (half, width), 1) < half
    gram_out[...] = jnp.where(keep, total[:half], total[half:])
    proj_out[...] = jnp.where(keep, total2[:half], total2[half:])

    for panel, name in ((p_panel, "p"), (s_panel, "s"), (m_panel, "m"), (b_panel, "b"), (t_panel, "t"), (i_panel, "i")):
        sent = panel.at[pl.ds(0, blocks - 1)]
        copy(sent, sent, sibling, (name + "a", "f", 1) if name in "pmt" else (name, "z")).wait_send()

    @pl.when(row != col)
    def _():
        to_mirror.wait_send()


def per_device(matrix, polar_factor, start_basis):
    width = start_basis.shape[0]
    blocks = 16
    vmem = pl.BlockSpec(memory_space=pltpu.VMEM)
    out = jax.ShapeDtypeStruct((width // 2, width), F32)
    panel = pltpu.VMEM((blocks, width, width), BF16)
    return pl.pallas_call(
        kernel,
        out_shape=(out, out),
        in_specs=[vmem] * 3,
        out_specs=(vmem, vmem),
        scratch_shapes=[panel] * 6
        + [
            pltpu.VMEM((width, width), BF16),
            pltpu.VMEM((width, width), F32),
            pltpu.VMEM((width, width), F32),
            pltpu.SemaphoreType.DMA((7,)),
            pltpu.SemaphoreType.DMA((N_SEMS,)),
        ],
        compiler_params=pltpu.CompilerParams(
            collective_id=0, has_side_effects=True, vmem_limit_bytes=48 * 1024 * 1024
        ),
    )(polar_factor, matrix, start_basis)


def solution(mesh):
    return jax.shard_map(
        per_device,
        mesh=mesh,
        in_specs=(P("row", "col"), P("row", "col"), P("row", "col")),
        out_specs=(P("row", "col"), P("row", "col")),
        check_vma=False,
    )
```
